32 devices in a mesh: fsdp: 4 (over z), model: 4 (over x, core), shift: 2 (over y).
Axes of the slice: x: 2, y: 2, z: 4, core: 2. Of those that a mesh axis runs over, the one named last changes fastest.
Arguments:
- w_query: float32 [9216, 4096], P(('shift', 'fsdp'), 'model'), parts along dimension 0, may hold values from -0.125 to 0.125
- first_query: float32 [9216, 4096], P(('shift', 'fsdp'), 'model'), parts along dimension 0, may hold values from -0.09375 to 0.09375
- second_query: float32 [9216, 4096], P(('shift', 'fsdp'), 'model'), parts along dimension 0, may hold values from -0.09375 to 0.09375
- w_key: float32 [9216, 2048], P(('shift', 'fsdp'), 'model'), parts along dimension 0, may hold values from -0.125 to 0.125
- first_key: float32 [9216, 2048], P(('shift', 'fsdp'), 'model'), parts along dimension 0, may hold values from -0.09375 to 0.09375
- second_key: float32 [9216, 2048], P(('shift', 'fsdp'), 'model'), parts along dimension 0, may hold values from -0.09375 to 0.09375
- w_value: float32 [9216, 2048], P(('shift', 'fsdp'), 'model'), parts along dimension 0, may hold values from -0.125 to 0.125
- first_value: float32 [9216, 2048], P(('shift', 'fsdp'), 'model'), parts along dimension 0, may hold values from -0.09375 to 0.09375
- second_value: float32 [9216, 2048], P(('shift', 'fsdp'), 'model'), parts along dimension 0, may hold values from -0.09375 to 0.09375
- norm_gain: float32 [9216], P(('shift', 'fsdp')), parts along dimension 0, may hold values from 0.25 to 1.75
Outputs:
- ready_query: bfloat16 [9216, 4096], P('shift', 'model'), parts along dimension 0
- ready_key: bfloat16 [9216, 2048], P('shift', 'model'), parts along dimension 0
- ready_value: bfloat16 [9216, 2048], P('shift', 'model'), parts along dimension 0
- scale_query: float32 [8192], P(('shift', 'model')), parts along dimension 0
- scale_key: float32 [4096], P(('shift', 'model')), parts along dimension 0
- scale_value: float32 [4096], P(('shift', 'model')), parts along dimension 0
The draws below stay inside these ranges and needn't reach their ends.
There are 2 independent parts, one for each index of `shift`. The reference program is written for one: setup_inputs(seed, part) draws one part's arguments, and reference() takes and returns one part's arrays. A program takes and returns all parts, laid end to end along the dimension named above; each array names one. Nothing has to cross between parts.
All inputs are finite; a program needn't handle non-finite values. Where the reference program divides by a largest or mean magnitude, that divisor is 1e-20 or more.
Results may differ from the reference program's by a relative error of at most 0.001.
Values may be sent and summed in bfloat16 or wider, within the bound.
A program may use at most 128 MiB of HBM per device.

```python
import jax
import jax.numpy as jnp

D_MODEL = 4608
Q_DIM = 4096
KV_DIM = 2048


def spiked(array, rng, source, target, blocks, factor):
    owner, partner = [(jnp.arange(array.shape[dim]) // (array.shape[dim] // blocks)).reshape([-1 if axis == dim else 1 for axis in range(array.ndim)]) for dim in (source, target)]
    chosen = jax.random.permutation(rng, blocks)[partner]
    strong = (owner == chosen) | (owner == (partner + blocks // 2) % blocks)
    return jnp.where(strong, factor * array, array)


def level_of(stream_key, shape, shards, low, high):
    factor_of, own = 1.0, jax.random.fold_in(stream_key, 6)
    for axis_at, parts in shards:
        heights = jnp.exp(jax.random.uniform(jax.random.fold_in(own, axis_at), (parts,), jnp.float32, low / len(shards), high / len(shards)))
        factor_of = factor_of * jnp.repeat(heights, shape[axis_at] // parts).reshape([-1 if axis == axis_at else 1 for axis in range(len(shape))])
    return factor_of


def centred(stream_key, dims, width, limit, shards=(), dtype=jnp.bfloat16):
    entries = jax.random.normal(stream_key, dims, jnp.float32) * width
    if len(shards) > 0:
        entries = level_of(stream_key, dims, shards, -0.22, 0.18) * entries
    return jnp.clip(entries, min=-limit, max=limit).astype(dtype)


def noise_with(key, extent, deviation, reach, shards, heavy, kind=jnp.bfloat16):
    entries = deviation * jax.random.normal(key, extent, jnp.float32)
    if shards:
        entries = entries * level_of(key, extent, shards, -0.22, 0.18)
    return jnp.clip(spiked(entries, jax.random.fold_in(key, 3), *heavy), -reach, reach).astype(kind)


def setup_inputs(seed: int = 0, part: int = 0) -> dict:
    splits = jax.random.split(jax.random.key(seed), 11)
    part_splits = jax.random.split(jax.random.fold_in(splits[10], part), 11)
    return {
        "w_query": noise_with(part_splits[0], (D_MODEL, Q_DIM), D_MODEL ** -0.5, 0.125, ((0, 4), (1, 4)), (0, 1, 4, 2.0), jnp.float32),
        "first_query": centred(part_splits[1], (D_MODEL, Q_DIM), D_MODEL ** -0.5, 0.09375, ((0, 4), (1, 4)), jnp.float32),
        "second_query": centred(part_splits[2], (D_MODEL, Q_DIM), D_MODEL ** -0.5, 0.09375, ((0, 4), (1, 4)), jnp.float32),
        "w_key": noise_with(part_splits[3], (D_MODEL, KV_DIM), D_MODEL ** -0.5, 0.125, ((0, 4), (1, 4)), (0, 1, 4, 2.0), jnp.float32),
        "first_key": centred(part_splits[4], (D_MODEL, KV_DIM), D_MODEL ** -0.5, 0.09375, ((0, 4), (1, 4)), jnp.float32),
        "second_key": centred(part_splits[5], (D_MODEL, KV_DIM), D_MODEL ** -0.5, 0.09375, ((0, 4), (1, 4)), jnp.float32),
        "w_value": noise_with(part_splits[6], (D_MODEL, KV_DIM), D_MODEL ** -0.5, 0.125, ((0, 4), (1, 4)), (0, 1, 4, 2.0), jnp.float32),
        "first_value": centred(part_splits[7], (D_MODEL, KV_DIM), D_MODEL ** -0.5, 0.09375, ((0, 4), (1, 4)), jnp.float32),
        "second_value": centred(part_splits[8], (D_MODEL, KV_DIM), D_MODEL ** -0.5, 0.09375, ((0, 4), (1, 4)), jnp.float32),
        "norm_gain": jnp.clip(1.0 + 0.15 * jax.random.normal(part_splits[9], (D_MODEL,), jnp.float32), 0.25, 1.75),
    }


learn_rate = 0.2
hold_rate = 0.8


def reference(w_query, first_query, second_query, w_key, first_key, second_key, w_value, first_value, second_value, norm_gain):
    hold_query = hold_rate * first_query + second_query
    latest_query = w_query - learn_rate * hold_query
    hold_key = hold_rate * first_key + second_key
    latest_key = w_key - learn_rate * hold_key
    hold_value = hold_rate * first_value + second_value
    latest_value = w_value - learn_rate * hold_value
    latest_gained_query = latest_query * norm_gain[:, None]
    latest_gained_key = latest_key * norm_gain[:, None]
    latest_gained_value = latest_value * norm_gain[:, None]
    scale_query = jnp.max(jnp.abs(latest_gained_query), axis=0)
    ready_query = (latest_gained_query / scale_query).astype(jnp.bfloat16)
    scale_key = jnp.max(jnp.abs(latest_gained_key), axis=0)
    ready_key = (latest_gained_key / scale_key).astype(jnp.bfloat16)
    scale_value = jnp.max(jnp.abs(latest_gained_value), axis=0)
    ready_value = (latest_gained_value / scale_value).astype(jnp.bfloat16)
    return ready_query, ready_key, ready_value, scale_query, scale_key, scale_value
```

```python
import functools

import jax
import jax.numpy as jnp
from jax import lax
from jax.experimental import pallas as pl
from jax.experimental.pallas import tpu as pltpu
from jax.sharding import PartitionSpec as P

learn_rate = 0.2
hold_rate = 0.8
AXIS = "fsdp"
MESH = pl.DeviceIdType.MESH
LANES = 128
AHEAD = 2
LAG = 2


def tile_of(rows, most=64):
    return max(t for t in range(16, most + 1, 16) if rows % t == 0)


def width_of(columns, most=256):
    return max(t for t in range(LANES, most + 1, LANES) if columns % t == 0)


def gather_kernel(n, chunks, *refs):
    params, gain_ref = refs[:9], refs[9]
    ready, scales = refs[10:13], refs[13:16]
    bufs = refs[16:19]
    gain_wide, mine, theirs = refs[19:22]
    load_sem, max_send, max_recv, send_sem, back_sem, recv_sem = refs[22:]
    rows = params[0].shape[0]
    tile = tile_of(rows)
    me = lax.axis_index(AXIS)

    def loads(c):
        a, offset, width = chunks[c]
        return [
            pltpu.make_async_copy(
                params[3 * a + k].at[:, pl.ds(offset, width)],
                bufs[a].at[k, :, pl.ds(offset, width)],
                load_sem.at[c, k],
            )
            for k in range(3)
        ]

    for c in range(min(AHEAD, len(chunks))):
        for copy in loads(c):
            copy.start()

    barrier = pltpu.get_barrier_semaphore()

    def greet(k, carry):
        pl.semaphore_signal(
            barrier, inc=1, device_id={AXIS: lax.rem(me + k, n)}, device_id_type=MESH
        )
        return carry

    lax.fori_loop(1, n, greet, 0)

    for k in range(gain_ref.shape[0]):
        block = jnp.broadcast_to(gain_ref[pl.ds(k, 1), :], (LANES, LANES))
        gain_wide[pl.ds(k * LANES, LANES), :] = block.T

    pl.semaphore_wait(barrier, n - 1)

    def max_copy(c, k):
        width = chunks[c][2] // LANES
        return pltpu.make_async_remote_copy(
            src_ref=mine.at[c, pl.ds(0, width)],
            dst_ref=theirs.at[c, k - 1, pl.ds(0, width)],
            send_sem=max_send.at[c, k - 1],
            recv_sem=max_recv.at[c, k - 1],
            device_id={AXIS: lax.rem(me + k, n)},
            device_id_type=MESH,
        )

    def step(c):
        a, offset, width = chunks[c]
        for copy in loads(c):
            copy.wait()
        parts = width // LANES

        def some(i, tops):
            r = pl.ds(pl.multiple_of(i * tile, tile), tile)
            gain = gain_wide[r, :]
            new = []
            for h in range(parts):
                cols = pl.ds(offset + h * LANES, LANES)
                hold = hold_rate * bufs[a][1, r, cols] + bufs[a][2, r, cols]
                gained = (bufs[a][0, r, cols] - learn_rate * hold) * gain
                bufs[a][0, r, cols] = gained
                top = jnp.max(jnp.abs(gained).reshape(tile // 8, 8, LANES), axis=0)
                new.append(jnp.maximum(tops[h], top))
            return tuple(new)

        tops = lax.fori_loop(
            0, rows // tile, some, tuple(jnp.zeros((8, LANES), jnp.float32) for _ in range(parts))
        )
        for h in range(parts):
            mine[c, h] = tops[h]

    def tell(c):
        def one(k, carry):
            max_copy(c, k).start()
            return carry

        lax.fori_loop(1, n, one, 0)

    def piece(c, block, target, sem):
        a, offset, width = chunks[c]
        where = ready[a].at[pl.ds(pl.multiple_of(block * rows, 16), rows), pl.ds(offset, width)]
        return pltpu.make_async_remote_copy(
            src_ref=where,
            dst_ref=where,
            send_sem=sem,
            recv_sem=recv_sem.at[block, c],
            device_id={AXIS: target},
            device_id_type=MESH,
        )

    def rightward(c, block):
        return piece(c, block, me + 1, send_sem.at[block, c])

    def leftward(c, block):
        return piece(c, block, me - 1, send_sem.at[block, c])

    def own_leftward(c):
        return piece(c, me, me - 1, back_sem.at[c])

    def finish(c):
        a, offset, width = chunks[c]

        def hear(k, carry):
            max_copy(c, k).wait_recv()
            return carry

        lax.fori_loop(1, n, hear, 0)
        parts = width // LANES
        tops = []
        for h in range(parts):
            top = lax.fori_loop(
                0, n - 1, lambda k, t: jnp.maximum(t, theirs[c, k, h]), mine[c, h]
            )
            top = jnp.max(top, axis=0, keepdims=True)
            scales[a][pl.ds(offset // LANES + h, 1), :] = top
            tops.append(top)

        def some(i, carry):
            r = pl.ds(pl.multiple_of(i * tile, tile), tile)
            to = pl.ds(pl.multiple_of(me * rows + i * tile, 16), tile)
            for h in range(parts):
                cols = pl.ds(offset + h * LANES, LANES)
                ready[a][to, cols] = (bufs[a][0, r, cols] / tops[h]).astype(jnp.bfloat16)
            return carry

        lax.fori_loop(0, rows // tile, some, 0)

        @pl.when(me < n - 1)
        def _():
            rightward(c, me).start()

        @pl.when(me > 0)
        def _():
            own_leftward(c).start()

    total = len(chunks)
    for c in range(total + LAG):
        if c < total:
            step(c)
            if c + AHEAD < total:
                for copy in loads(c + AHEAD):
                    copy.start()
            tell(c)
        if c >= LAG:
            finish(c - LAG)

    def hop(s, carry):
        for c in range(total):

            @pl.when(me - s >= 0)
            def _():
                block = me - s
                rightward(c, block).wait_recv()

                @pl.when(me < n - 1)
                def _():
                    rightward(c, block).start()

            @pl.when(me + s < n)
            def _():
                block = me + s
                leftward(c, block).wait_recv()

                @pl.when(me > 0)
                def _():
                    leftward(c, block).start()

        return carry

    lax.fori_loop(1, n, hop, 0)

    def close(s, carry):
        for c in range(total):

            @pl.when((me - s >= 0) & (me < n - 1))
            def _():
                rightward(c, me - s).wait_send()

            @pl.when((me + s < n) & (me > 0) & (s > 0))
            def _():
                leftward(c, me + s).wait_send()

        return carry

    lax.fori_loop(0, n, close, 0)
    for c in range(total):

        @pl.when(me > 0)
        def _():
            own_leftward(c).wait_send()

        def sent(k, carry):
            max_copy(c, k).wait_send()
            return carry

        lax.fori_loop(1, n, sent, 0)


def store_kernel(cuts, *refs):
    sources, targets, sem = refs[:6], refs[6:12], refs[12]
    copies = []
    for a in range(6):
        pieces = cuts if a < 3 else 1
        height = sources[a].shape[0] // pieces
        for k in range(pieces):
            part = pl.ds(k * height, height)
            copies.append(
                pltpu.make_async_copy(sources[a].at[part], targets[a].at[part], sem.at[a, k])
            )
    for copy in copies:
        copy.start()
    for copy in copies:
        copy.wait()


def body(n, *args):
    params, gain = args[:9], args[9]
    rows = params[0].shape[0]
    widths = [params[3 * a].shape[1] for a in range(3)]
    chunks = []
    for a in (1, 2, 0):
        width = width_of(widths[a])
        chunks += [(a, offset, width) for offset in range(0, widths[a], width)]
    total = len(chunks)
    wide = max(width for _, _, width in chunks) // LANES
    groups = -(-rows // LANES)
    if groups * LANES != rows:
        gain = jnp.pad(gain, (0, groups * LANES - rows))
    gain = gain.reshape(groups, LANES)
    shapes = [((n * rows, width), jnp.bfloat16) for width in widths]
    shapes += [((width // LANES, LANES), jnp.float32) for width in widths]
    gathered = pl.pallas_call(
        functools.partial(gather_kernel, n, tuple(chunks)),
        out_shape=[pltpu.VMEM(shape, dtype) for shape, dtype in shapes],
        in_specs=[pl.BlockSpec(memory_space=pl.ANY)] * 9 + [pl.BlockSpec(memory_space=pltpu.VMEM)],
        out_specs=[pl.BlockSpec(memory_space=pltpu.VMEM)] * 6,
        scratch_shapes=[pltpu.VMEM((3, rows, width), jnp.float32) for width in widths]
        + [
            pltpu.VMEM((groups * LANES, LANES), jnp.float32),
            pltpu.VMEM((total, wide, 8, LANES), jnp.float32),
            pltpu.VMEM((total, n - 1, wide, 8, LANES), jnp.float32),
            pltpu.SemaphoreType.DMA((total, 3)),
            pltpu.SemaphoreType.DMA((total, n - 1)),
            pltpu.SemaphoreType.DMA((total, n - 1)),
            pltpu.SemaphoreType.DMA((n, total)),
            pltpu.SemaphoreType.DMA((total,)),
            pltpu.SemaphoreType.DMA((n, total)),
        ],
        compiler_params=pltpu.CompilerParams(
            collective_id=0, has_side_effects=True, vmem_limit_bytes=40 * 2**20
        ),
        name="gather",
    )(*params, gain)
    cuts = 4
    stored = pl.pallas_call(
        functools.partial(store_kernel, cuts),
        out_shape=[jax.ShapeDtypeStruct(shape, dtype) for shape, dtype in shapes],
        in_specs=[pl.BlockSpec(memory_space=pltpu.VMEM)] * 6,
        out_specs=[pl.BlockSpec(memory_space=pl.ANY)] * 6,
        scratch_shapes=[pltpu.SemaphoreType.DMA((6, cuts))],
        compiler_params=pltpu.CompilerParams(vmem_limit_bytes=2**20),
        name="store",
    )(*gathered)
    return (*stored[:3], *(s.reshape(-1) for s in stored[3:]))


def solution(mesh):
    matrix = P(("shift", AXIS), "model")
    column = P(("shift", "model"))
    whole = P("shift", "model")
    return jax.shard_map(
        functools.partial(body, mesh.shape[AXIS]),
        mesh=mesh,
        in_specs=(matrix,) * 9 + (P(("shift", AXIS)),),
        out_specs=(whole, whole, whole, column, column, column),
        check_vma=False,
    )
```

```python
import functools

import jax
import jax.numpy as jnp
from jax import lax
from jax.experimental import pallas as pl
from jax.experimental.pallas import tpu as pltpu
from jax.sharding import PartitionSpec as P

learn_rate = 0.2
hold_rate = 0.8
AXIS = "fsdp"
MESH = pl.DeviceIdType.MESH
LANES = 128
AHEAD = 2
LAG = 2


def tile_of(rows, most=64):
    return max(t for t in range(16, most + 1, 16) if rows % t == 0)


def width_of(columns, most=256):
    return max(t for t in range(LANES, most + 1, LANES) if columns % t == 0)


def gather_kernel(n, chunks, *refs):
    params, gain_ref = refs[:9], refs[9]
    ready, scales, last = refs[10:13], refs[13:16], refs[16]
    bufs = refs[17:20]
    gain_wide, mine, theirs = refs[20:23]
    load_sem, max_send, max_recv, send_sem, back_sem, recv_sem, last_sem = refs[23:]
    total = len(chunks)
    rows = params[0].shape[0]
    tile = tile_of(rows)
    me = lax.axis_index(AXIS)

    def loads(c):
        a, offset, width = chunks[c]
        return [
            pltpu.make_async_copy(
                params[3 * a + k].at[:, pl.ds(offset, width)],
                bufs[a].at[k, :, pl.ds(offset, width)],
                load_sem.at[c, k],
            )
            for k in range(3)
        ]

    for copy in loads(0):
        copy.start()

    barrier = pltpu.get_barrier_semaphore()

    def greet(k, carry):
        pl.semaphore_signal(
            barrier, inc=1, device_id={AXIS: lax.rem(me + k, n)}, device_id_type=MESH
        )
        return carry

    lax.fori_loop(1, n, greet, 0)

    for c in range(1, min(AHEAD, len(chunks))):
        for copy in loads(c):
            copy.start()

    for k in range(gain_ref.shape[0]):
        block = jnp.broadcast_to(gain_ref[pl.ds(k, 1), :], (LANES, LANES))
        gain_wide[pl.ds(k * LANES, LANES), :] = block.T

    def max_copy(c, k):
        width = chunks[c][2] // LANES
        return pltpu.make_async_remote_copy(
            src_ref=mine.at[c, pl.ds(0, width)],
            dst_ref=theirs.at[c, k - 1, pl.ds(0, width)],
            send_sem=max_send.at[c, k - 1],
            recv_sem=max_recv.at[c, k - 1],
            device_id={AXIS: lax.rem(me + k, n)},
            device_id_type=MESH,
        )

    def step(c):
        a, offset, width = chunks[c]
        for copy in loads(c):
            copy.wait()
        parts = width // LANES

        def some(i, tops):
            r = pl.ds(pl.multiple_of(i * tile, tile), tile)
            gain = gain_wide[r, :]
            new = []
            for h in range(parts):
                cols = pl.ds(offset + h * LANES, LANES)
                hold = hold_rate * bufs[a][1, r, cols] + bufs[a][2, r, cols]
                gained = (bufs[a][0, r, cols] - learn_rate * hold) * gain
                bufs[a][0, r, cols] = gained
                top = jnp.max(jnp.abs(gained).reshape(tile // 8, 8, LANES), axis=0)
                new.append(jnp.maximum(tops[h], top))
            return tuple(new)

        tops = lax.fori_loop(
            0, rows // tile, some, tuple(jnp.zeros((8, LANES), jnp.float32) for _ in range(parts))
        )
        for h in range(parts):
            mine[c, h] = tops[h]

    def tell(c):
        def one(k, carry):
            max_copy(c, k).start()
            return carry

        lax.fori_loop(1, n, one, 0)

    def piece(c, block, target, sem):
        a, offset, width = chunks[c]
        where = ready[a].at[pl.ds(pl.multiple_of(block * rows, 16), rows), pl.ds(offset, width)]
        return pltpu.make_async_remote_copy(
            src_ref=where,
            dst_ref=where,
            send_sem=sem,
            recv_sem=recv_sem.at[block, c],
            device_id={AXIS: target},
            device_id_type=MESH,
        )

    def rightward(c, block):
        return piece(c, block, me + 1, send_sem.at[block, c])

    def leftward(c, block):
        return piece(c, block, me - 1, send_sem.at[block, c])

    def own_leftward(c):
        return piece(c, me, me - 1, back_sem.at[c])

    def goes_right(c):
        return (me < n - 2) if c == total - 1 else (me < n - 1)

    def goes_left(c):
        return (me > 1) if c == total - 1 else (me > 0)

    def keep():
        a, offset, width = chunks[-1]
        own = ready[a].at[pl.ds(pl.multiple_of(me * rows, 16), rows), pl.ds(offset, width)]
        return pltpu.make_async_copy(own, last, last_sem)

    def finish(c):
        a, offset, width = chunks[c]

        def hear(k, carry):
            max_copy(c, k).wait_recv()
            return carry

        lax.fori_loop(1, n, hear, 0)
        parts = width // LANES
        tops = []
        for h in range(parts):
            top = lax.fori_loop(
                0, n - 1, lambda k, t: jnp.maximum(t, theirs[c, k, h]), mine[c, h]
            )
            top = jnp.max(top, axis=0, keepdims=True)
            scales[a][pl.ds(offset // LANES + h, 1), :] = top
            tops.append(top)

        def some(i, carry):
            r = pl.ds(pl.multiple_of(i * tile, tile), tile)
            to = pl.ds(pl.multiple_of(me * rows + i * tile, 16), tile)
            for h in range(parts):
                cols = pl.ds(offset + h * LANES, LANES)
                ready[a][to, cols] = (bufs[a][0, r, cols] / tops[h]).astype(jnp.bfloat16)
            return carry

        lax.fori_loop(0, rows // tile, some, 0)

        if c == total - 1:
            keep().start()

        @pl.when(goes_right(c))
        def _():
            rightward(c, me).start()

        @pl.when(goes_left(c))
        def _():
            own_leftward(c).start()

    for c in range(total + LAG):
        if c < total:
            step(c)
            if c + AHEAD < total:
                for copy in loads(c + AHEAD):
                    copy.start()
            if c == 0:
                pl.semaphore_wait(barrier, n - 1)
            tell(c)
        if c >= LAG:
            finish(c - LAG)

    def hop(s, carry):
        for c in range(total):

            from_left, from_right = me - s >= 0, me + s < n
            if c == total - 1:
                from_left &= (me < n - 1) | (s > 1)
                from_right &= (me > 0) | (s > 1)

            @pl.when(from_left)
            def _():
                block = me - s
                rightward(c, block).wait_recv()

                @pl.when(me < n - 1)
                def _():
                    rightward(c, block).start()

            @pl.when(from_right)
            def _():
                block = me + s
                leftward(c, block).wait_recv()

                @pl.when(me > 0)
                def _():
                    leftward(c, block).start()

        return carry

    lax.fori_loop(1, n, hop, 0)

    def close(s, carry):
        for c in range(total):

            to_right = (me - s >= 0) & (me < n - 1)
            if c == total - 1:
                to_right &= (me < n - 2) | (s > 0)

            @pl.when(to_right)
            def _():
                rightward(c, me - s).wait_send()

            @pl.when((me + s < n) & (me > 0) & (s > 0))
            def _():
                leftward(c, me + s).wait_send()

        return carry

    lax.fori_loop(0, n, close, 0)
    keep().wait()
    for c in range(total):

        @pl.when(goes_left(c))
        def _():
            own_leftward(c).wait_send()

        def sent(k, carry):
            max_copy(c, k).wait_send()
            return carry

        lax.fori_loop(1, n, sent, 0)


def store_kernel(cuts, *refs):
    sources, targets, sem = refs[:6], refs[6:12], refs[12]
    copies = []
    for a in range(6):
        pieces = cuts if a < 3 else 1
        height = sources[a].shape[0] // pieces
        for k in range(pieces):
            part = pl.ds(k * height, height)
            copies.append(
                pltpu.make_async_copy(sources[a].at[part], targets[a].at[part], sem.at[a, k])
            )
    for copy in copies:
        copy.start()
    for copy in copies:
        copy.wait()


def patch_kernel(n, offset, old_ref, piece_ref, new_ref, sem):
    del old_ref
    rows, width = piece_ref.shape
    me = lax.axis_index(AXIS)

    @pl.when((me == 0) | (me == n - 1))
    def _():
        block = jnp.where(me == 0, 1, n - 2)
        copy = pltpu.make_async_copy(
            piece_ref,
            new_ref.at[pl.ds(pl.multiple_of(block * rows, 16), rows), pl.ds(offset, width)],
            sem,
        )
        copy.start()
        copy.wait()


def body(n, *args):
    params, gain = args[:9], args[9]
    rows = params[0].shape[0]
    widths = [params[3 * a].shape[1] for a in range(3)]
    chunks = []
    for a in (1, 2, 0):
        width = width_of(widths[a])
        chunks += [(a, offset, width) for offset in range(0, widths[a], width)]
    a, offset, width = chunks[0]
    chunks[:1] = [(a, offset + part, LANES) for part in range(0, width, LANES)]
    a, offset, width = chunks[-1]
    chunks[-1:] = [(a, offset + part, LANES) for part in range(0, width, LANES)]
    total = len(chunks)
    last_array, last_offset, last_width = chunks[-1]
    wide = max(width for _, _, width in chunks) // LANES
    groups = -(-rows // LANES)
    if groups * LANES != rows:
        gain = jnp.pad(gain, (0, groups * LANES - rows))
    gain = gain.reshape(groups, LANES)
    shapes = [((n * rows, width), jnp.bfloat16) for width in widths]
    shapes += [((width // LANES, LANES), jnp.float32) for width in widths]
    gathered = pl.pallas_call(
        functools.partial(gather_kernel, n, tuple(chunks)),
        out_shape=[pltpu.VMEM(shape, dtype) for shape, dtype in shapes]
        + [jax.ShapeDtypeStruct((rows, last_width), jnp.bfloat16)],
        in_specs=[pl.BlockSpec(memory_space=pl.ANY)] * 9 + [pl.BlockSpec(memory_space=pltpu.VMEM)],
        out_specs=[pl.BlockSpec(memory_space=pltpu.VMEM)] * 6 + [pl.BlockSpec(memory_space=pl.ANY)],
        scratch_shapes=[pltpu.VMEM((3, rows, width), jnp.float32) for width in widths]
        + [
            pltpu.VMEM((groups * LANES, LANES), jnp.float32),
            pltpu.VMEM((total, wide, 8, LANES), jnp.float32),
            pltpu.VMEM((total, n - 1, wide, 8, LANES), jnp.float32),
            pltpu.SemaphoreType.DMA((total, 3)),
            pltpu.SemaphoreType.DMA((total, n - 1)),
            pltpu.SemaphoreType.DMA((total, n - 1)),
            pltpu.SemaphoreType.DMA((n, total)),
            pltpu.SemaphoreType.DMA((total,)),
            pltpu.SemaphoreType.DMA((n, total)),
            pltpu.SemaphoreType.DMA,
        ],
        compiler_params=pltpu.CompilerParams(
            collective_id=0, has_side_effects=True, vmem_limit_bytes=40 * 2**20
        ),
        name="gather",
    )(*params, gain)
    *gathered, last = gathered
    piece = lax.ppermute(last, AXIS, ((n - 2, n - 1), (1, 0)))
    cuts = 4
    stored = pl.pallas_call(
        functools.partial(store_kernel, cuts),
        out_shape=[jax.ShapeDtypeStruct(shape, dtype) for shape, dtype in shapes],
        in_specs=[pl.BlockSpec(memory_space=pltpu.VMEM)] * 6,
        out_specs=[pl.BlockSpec(memory_space=pl.ANY)] * 6,
        scratch_shapes=[pltpu.SemaphoreType.DMA((6, cuts))],
        compiler_params=pltpu.CompilerParams(vmem_limit_bytes=2**20),
        cost_estimate=pl.CostEstimate(flops=0, bytes_accessed=4 * n * rows * sum(widths), transcendentals=0),
        name="store",
    )(*gathered)
    stored = list(stored)
    shape, dtype = shapes[last_array]
    stored[last_array] = pl.pallas_call(
        functools.partial(patch_kernel, n, last_offset),
        out_shape=jax.ShapeDtypeStruct(shape, dtype),
        in_specs=[pl.BlockSpec(memory_space=pl.ANY), pl.BlockSpec(memory_space=pltpu.VMEM)],
        out_specs=pl.BlockSpec(memory_space=pl.ANY),
        scratch_shapes=[pltpu.SemaphoreType.DMA],
        input_output_aliases={0: 0},
        compiler_params=pltpu.CompilerParams(vmem_limit_bytes=2**20),
        name="patch",
    )(stored[last_array], piece)
    return (*stored[:3], *(s.reshape(-1) for s in stored[3:]))


def solution(mesh):
    matrix = P(("shift", AXIS), "model")
    column = P(("shift", "model"))
    whole = P("shift", "model")
    return jax.shard_map(
        functools.partial(body, mesh.shape[AXIS]),
        mesh=mesh,
        in_specs=(matrix,) * 9 + (P(("shift", AXIS)),),
        out_specs=(whole, whole, whole, column, column, column),
        check_vma=False,
    )
```

```python
import functools

import jax
import jax.numpy as jnp
from jax import lax
from jax.experimental import pallas as pl
from jax.experimental.pallas import tpu as pltpu
from jax.sharding import PartitionSpec as P

learn_rate = 0.2
hold_rate = 0.8
AXIS = "fsdp"
MESH = pl.DeviceIdType.MESH
LANES = 128
AHEAD = 2
LAG = 1


def tile_of(rows, most=64):
    return max(t for t in range(16, most + 1, 16) if rows % t == 0)


def width_of(columns, most=256):
    return max(t for t in range(LANES, most + 1, LANES) if columns % t == 0)


def gather_kernel(n, chunks, *refs):
    params, gain_hbm = refs[:9], refs[9]
    ready, scales, last = refs[10:13], refs[13:16], refs[16]
    bufs = refs[17:20]
    gain_wide, mine, theirs = refs[20:23]
    load_sem, max_send, max_recv, send_sem, back_sem, recv_sem, last_sem, gain_ref, gain_sem = refs[23:]
    total = len(chunks)
    rows = params[0].shape[0]
    tile = tile_of(rows)
    me = lax.axis_index(AXIS)

    def loads(c):
        a, offset, width = chunks[c]
        return [
            pltpu.make_async_copy(
                params[3 * a + k].at[:, pl.ds(offset, width)],
                bufs[a].at[k, :, pl.ds(offset, width)],
                load_sem.at[c, k],
            )
            for k in range(3)
        ]

    gain_load = pltpu.make_async_copy(gain_hbm, gain_ref, gain_sem)
    gain_load.start()
    for copy in loads(0):
        copy.start()

    barrier = pltpu.get_barrier_semaphore()

    def greet(k, carry):
        pl.semaphore_signal(
            barrier, inc=1, device_id={AXIS: lax.rem(me + k, n)}, device_id_type=MESH
        )
        return carry

    lax.fori_loop(1, n, greet, 0)

    gain_load.wait()
    for k in range(gain_ref.shape[0]):
        block = jnp.broadcast_to(gain_ref[pl.ds(k, 1), :], (LANES, LANES))
        gain_wide[pl.ds(k * LANES, LANES), :] = block.T

    for c in range(1, min(AHEAD, total)):
        for copy in loads(c):
            copy.start()

    def max_copy(c, k):
        width = chunks[c][2] // LANES
        return pltpu.make_async_remote_copy(
            src_ref=mine.at[c, pl.ds(0, width)],
            dst_ref=theirs.at[c, k - 1, pl.ds(0, width)],
            send_sem=max_send.at[c, k - 1],
            recv_sem=max_recv.at[c, k - 1],
            device_id={AXIS: lax.rem(me + k, n)},
            device_id_type=MESH,
        )

    def step(c):
        a, offset, width = chunks[c]
        for copy in loads(c):
            copy.wait()
        parts = width // LANES

        def some(i, tops):
            r = pl.ds(pl.multiple_of(i * tile, tile), tile)
            gain = gain_wide[r, :]
            new = []
            for h in range(parts):
                cols = pl.ds(offset + h * LANES, LANES)
                hold = hold_rate * bufs[a][1, r, cols] + bufs[a][2, r, cols]
                gained = (bufs[a][0, r, cols] - learn_rate * hold) * gain
                bufs[a][0, r, cols] = gained
                top = jnp.max(jnp.abs(gained).reshape(tile // 8, 8, LANES), axis=0)
                new.append(jnp.maximum(tops[h], top))
            return tuple(new)

        tops = lax.fori_loop(
            0, rows // tile, some, tuple(jnp.zeros((8, LANES), jnp.float32) for _ in range(parts))
        )
        for h in range(parts):
            mine[c, h] = tops[h]

    def tell(c):
        def one(k, carry):
            max_copy(c, k).start()
            return carry

        lax.fori_loop(1, n, one, 0)

    def piece(c, block, target, sem):
        a, offset, width = chunks[c]
        where = ready[a].at[pl.ds(pl.multiple_of(block * rows, 16), rows), pl.ds(offset, width)]
        return pltpu.make_async_remote_copy(
            src_ref=where,
            dst_ref=where,
            send_sem=sem,
            recv_sem=recv_sem.at[block, c],
            device_id={AXIS: target},
            device_id_type=MESH,
        )

    def rightward(c, block):
        return piece(c, block, me + 1, send_sem.at[block, c])

    def leftward(c, block):
        return piece(c, block, me - 1, send_sem.at[block, c])

    def own_leftward(c):
        return piece(c, me, me - 1, back_sem.at[c])

    def goes_right(c):
        return (me < n - 2) if c == total - 1 else (me < n - 1)

    def goes_left(c):
        return (me > 1) if c == total - 1 else (me > 0)

    def keep():
        a, offset, width = chunks[-1]
        own = ready[a].at[pl.ds(pl.multiple_of(me * rows, 16), rows), pl.ds(offset, width)]
        return pltpu.make_async_copy(own, last, last_sem)

    def finish(c):
        a, offset, width = chunks[c]

        def hear(k, carry):
            max_copy(c, k).wait_recv()
            return carry

        lax.fori_loop(1, n, hear, 0)
        parts = width // LANES
        tops = []
        for h in range(parts):
            top = lax.fori_loop(
                0, n - 1, lambda k, t: jnp.maximum(t, theirs[c, k, h]), mine[c, h]
            )
            top = jnp.max(top, axis=0, keepdims=True)
            scales[a][pl.ds(offset // LANES + h, 1), :] = top
            tops.append(top)

        def some(i, carry):
            r = pl.ds(pl.multiple_of(i * tile, tile), tile)
            to = pl.ds(pl.multiple_of(me * rows + i * tile, 16), tile)
            for h in range(parts):
                cols = pl.ds(offset + h * LANES, LANES)
                ready[a][to, cols] = (bufs[a][0, r, cols] / tops[h]).astype(jnp.bfloat16)
            return carry

        lax.fori_loop(0, rows // tile, some, 0)

        if c == total - 1:
            keep().start()

        @pl.when(goes_right(c))
        def _():
            rightward(c, me).start()

        @pl.when(goes_left(c))
        def _():
            own_leftward(c).start()

    for c in range(total + LAG):
        if c < total:
            step(c)
            if c + AHEAD < total:
                for copy in loads(c + AHEAD):
                    copy.start()
            if c == 0:
                pl.semaphore_wait(barrier, n - 1)
            tell(c)
        if c >= LAG:
            finish(c - LAG)

    def sent(c, s):
        to_right = (me - s >= 0) & (me < n - 1)
        to_left = (me + s < n) & (me > 0) & (s > 0)
        if c == total - 1:
            to_right &= (me < n - 2) | (s > 0)

        @pl.when(to_right)
        def _():
            rightward(c, me - s).wait_send()

        @pl.when(to_left)
        def _():
            leftward(c, me + s).wait_send()

    for c in range(total):

        def told(k, carry):
            max_copy(c, k).wait_send()
            return carry

        lax.fori_loop(1, n, told, 0)
    keep().wait()

    def hop(s, carry):
        for c in range(total):
            from_left, from_right = me - s >= 0, me + s < n
            if c == total - 1:
                from_left &= (me < n - 1) | (s > 1)
                from_right &= (me > 0) | (s > 1)

            @pl.when(from_left)
            def _():
                block = me - s
                rightward(c, block).wait_recv()

                @pl.when(me < n - 1)
                def _():
                    rightward(c, block).start()

            @pl.when(from_right)
            def _():
                block = me + s
                leftward(c, block).wait_recv()

                @pl.when(me > 0)
                def _():
                    leftward(c, block).start()

            sent(c, s - 1)

            @pl.when(goes_left(c) & (s == 1))
            def _():
                own_leftward(c).wait_send()

        return carry

    lax.fori_loop(1, n, hop, 0)
    for c in range(total):
        sent(c, n - 1)


def store_kernel(cuts, *refs):
    sources, targets, sem = refs[:6], refs[6:12], refs[12]
    copies = []
    for a in range(6):
        pieces = cuts if a < 3 else 1
        height = sources[a].shape[0] // pieces
        for k in range(pieces):
            part = pl.ds(k * height, height)
            copies.append(
                pltpu.make_async_copy(sources[a].at[part], targets[a].at[part], sem.at[a, k])
            )
    for copy in copies:
        copy.start()
    for copy in copies:
        copy.wait()


def patch_kernel(n, offset, old_ref, piece_ref, new_ref, sem):
    del old_ref
    rows, width = piece_ref.shape
    me = lax.axis_index(AXIS)

    @pl.when((me == 0) | (me == n - 1))
    def _():
        block = jnp.where(me == 0, 1, n - 2)
        copy = pltpu.make_async_copy(
            piece_ref,
            new_ref.at[pl.ds(pl.multiple_of(block * rows, 16), rows), pl.ds(offset, width)],
            sem,
        )
        copy.start()
        copy.wait()


def body(n, *args):
    params, gain = args[:9], args[9]
    rows = params[0].shape[0]
    widths = [params[3 * a].shape[1] for a in range(3)]
    chunks = []
    for a in (1, 2, 0):
        width = width_of(widths[a])
        chunks += [(a, offset, width) for offset in range(0, widths[a], width)]
    a, offset, width = chunks[0]
    chunks[:1] = [(a, offset + part, LANES) for part in range(0, width, LANES)]
    a, offset, width = chunks[-1]
    chunks[-1:] = [(a, offset + part, LANES) for part in range(0, width, LANES)]
    total = len(chunks)
    last_array, last_offset, last_width = chunks[-1]
    wide = max(width for _, _, width in chunks) // LANES
    groups = -(-rows // LANES)
    if groups * LANES != rows:
        gain = jnp.pad(gain, (0, groups * LANES - rows))
    gain = gain.reshape(groups, LANES)
    shapes = [((n * rows, width), jnp.bfloat16) for width in widths]
    shapes += [((width // LANES, LANES), jnp.float32) for width in widths]
    gathered = pl.pallas_call(
        functools.partial(gather_kernel, n, tuple(chunks)),
        out_shape=[pltpu.VMEM(shape, dtype) for shape, dtype in shapes]
        + [jax.ShapeDtypeStruct((rows, last_width), jnp.bfloat16)],
        in_specs=[pl.BlockSpec(memory_space=pl.ANY)] * 10,
        out_specs=[pl.BlockSpec(memory_space=pltpu.VMEM)] * 6 + [pl.BlockSpec(memory_space=pl.ANY)],
        scratch_shapes=[pltpu.VMEM((3, rows, width), jnp.float32) for width in widths]
        + [
            pltpu.VMEM((groups * LANES, LANES), jnp.float32),
            pltpu.VMEM((total, wide, 8, LANES), jnp.float32),
            pltpu.VMEM((total, n - 1, wide, 8, LANES), jnp.float32),
            pltpu.SemaphoreType.DMA((total, 3)),
            pltpu.SemaphoreType.DMA((total, n - 1)),
            pltpu.SemaphoreType.DMA((total, n - 1)),
            pltpu.SemaphoreType.DMA((n, total)),
            pltpu.SemaphoreType.DMA((total,)),
            pltpu.SemaphoreType.DMA((n, total)),
            pltpu.SemaphoreType.DMA,
            pltpu.VMEM((groups, LANES), jnp.float32),
            pltpu.SemaphoreType.DMA,
        ],
        compiler_params=pltpu.CompilerParams(
            collective_id=0, has_side_effects=True, vmem_limit_bytes=40 * 2**20
        ),
        name="gather",
    )(*params, gain)
    *gathered, last = gathered
    piece = lax.ppermute(last, AXIS, ((n - 2, n - 1), (1, 0)))
    cuts = 4
    stored = pl.pallas_call(
        functools.partial(store_kernel, cuts),
        out_shape=[jax.ShapeDtypeStruct(shape, dtype) for shape, dtype in shapes],
        in_specs=[pl.BlockSpec(memory_space=pltpu.VMEM)] * 6,
        out_specs=[pl.BlockSpec(memory_space=pl.ANY)] * 6,
        scratch_shapes=[pltpu.SemaphoreType.DMA((6, cuts))],
        compiler_params=pltpu.CompilerParams(vmem_limit_bytes=2**20),
        cost_estimate=pl.CostEstimate(flops=0, bytes_accessed=4 * n * rows * sum(widths), transcendentals=0),
        name="store",
    )(*gathered)
    stored = list(stored)
    shape, dtype = shapes[last_array]
    stored[last_array] = pl.pallas_call(
        functools.partial(patch_kernel, n, last_offset),
        out_shape=jax.ShapeDtypeStruct(shape, dtype),
        in_specs=[pl.BlockSpec(memory_space=pl.ANY), pl.BlockSpec(memory_space=pltpu.VMEM)],
        out_specs=pl.BlockSpec(memory_space=pl.ANY),
        scratch_shapes=[pltpu.SemaphoreType.DMA],
        input_output_aliases={0: 0},
        compiler_params=pltpu.CompilerParams(vmem_limit_bytes=2**20),
        name="patch",
    )(stored[last_array], piece)
    return (*stored[:3], *(s.reshape(-1) for s in stored[3:]))


def solution(mesh):
    matrix = P(("shift", AXIS), "model")
    column = P(("shift", "model"))
    whole = P("shift", "model")
    return jax.shard_map(
        functools.partial(body, mesh.shape[AXIS]),
        mesh=mesh,
        in_specs=(matrix,) * 9 + (P(("shift", AXIS)),),
        out_specs=(whole, whole, whole, column, column, column),
        check_vma=False,
    )
```
